32 devices in a mesh: ia: 2 (over x), ja: 4 (over z), ka: 4 (over y, core).
Axes of the slice: x: 2, y: 2, z: 4, core: 2. Of those that a mesh axis runs over, the one named last changes fastest.
Arguments:
- tensor: bfloat16 [128, 256, 2, 512], P('ia', 'ja', None, 'ka'), may hold values from -6 to 6
- factor_two: float32 [256, 32], P('ja'), may hold values from -2 to 2
- factor_three: float32 [512, 32], P('ka'), may hold values from -2 to 2
- factor_four: float32 [2, 32], replicated, may hold values from -2 to 2
Outputs:
- new_one: float32 [128, 32], P('ia')
- new_two: float32 [256, 32], P('ja')
The draws below stay inside these ranges and needn't reach their ends.
All inputs are finite; a program needn't handle non-finite values.
Results may differ from the reference program's by a relative error of at most 0.0042.
Values sent between devices are 32-bit elements; how exact they have to be, the bound alone decides.
A program may use at most 64 MiB of HBM per device.

```python
import math
import jax
import jax.numpy as jnp
from jax import lax

RANK = 32
FOURTH = 2
DIM_ONE = 128
DIM_TWO = 256
DIM_THREE = 512


def loguniform_draw(key, extent, lowest, highest):
    return jnp.exp(jax.random.uniform(key, extent, jnp.float32, math.log(lowest), math.log(highest)))


def log_mean_square(lowest, highest):
    return (highest * highest - lowest * lowest) / (2.0 * math.log(highest / lowest))


def correlated_factor(key, row_count):
    subkeys = jax.random.split(key, 4)
    common_weight = 1.2
    column_lowest = 0.6
    column_highest = 1.4
    row_lowest = 0.3
    row_highest = 3.0
    noise = jax.random.truncated_normal(subkeys[0], -3.0, 3.0, (row_count, RANK), jnp.float32)
    common = jax.random.truncated_normal(subkeys[1], -3.0, 3.0, (row_count, 1), jnp.float32)
    column = loguniform_draw(subkeys[2], (1, RANK), column_lowest, column_highest)
    row_scale = loguniform_draw(subkeys[3], (row_count, 1), row_lowest, row_highest)
    spread = log_mean_square(row_lowest, row_highest) * (1.0 + common_weight * common_weight * log_mean_square(column_lowest, column_highest))
    return row_scale * (noise + common_weight * common * column) / math.sqrt(row_count * spread)


def draw_factor_two(key, part):
    return correlated_factor(jax.random.fold_in(key, 21), DIM_TWO)


def draw_factor_three(key, part):
    return correlated_factor(jax.random.fold_in(key, 22), DIM_THREE)


def draw_factor_four(key, part):
    subkeys = jax.random.split(jax.random.fold_in(key, 23), 2)
    signs = (2 * jax.random.randint(subkeys[0], (FOURTH, 1), 0, 2) - 1).astype(jnp.float32)
    magnitude = jax.random.uniform(subkeys[1], (FOURTH, RANK), jnp.float32, 0.5, 1.5)
    return signs * magnitude / math.sqrt(FOURTH)


def level_of(rng, shape, pieces, least, top_value):
    level = 1.0
    for dim, parts in pieces:
        draws = jax.random.uniform(jax.random.fold_in(jax.random.fold_in(rng, 6), dim), (parts,), jnp.float32, least / len(pieces), top_value / len(pieces))
        level = level * jnp.repeat(jnp.exp(draws), shape[dim] // parts).reshape((-1,) + (1,) * (len(shape) - 1 - dim))
    return level


def gaussian(key, dims, scale, reach, cuts=(), dtype=jnp.bfloat16):
    values = scale * jax.random.normal(key, dims, jnp.float32)
    if cuts:
        values = values * level_of(key, dims, cuts, -0.22, 0.18)
    return jnp.clip(values, -reach, reach).astype(dtype)


def setup_inputs(seed: int = 0) -> dict:
    arg_keys = jax.random.split(jax.random.key(seed), 5)
    tensor = gaussian(arg_keys[0], (DIM_ONE, DIM_TWO, FOURTH, DIM_THREE), 1.0, 6.0, ((0, 2), (1, 4), (3, 4)))
    factor_two = draw_factor_two(jax.random.fold_in(arg_keys[4], 71), 0)
    factor_three = draw_factor_three(jax.random.fold_in(arg_keys[4], 71), 0)
    factor_four = draw_factor_four(jax.random.fold_in(arg_keys[4], 71), 0)
    return {"tensor": tensor, "factor_two": factor_two, "factor_three": factor_three, "factor_four": factor_four}


def solve_rows(rhs, system):
    lower = jnp.linalg.cholesky(system)
    return jax.scipy.linalg.cho_solve((lower, True), rhs.T).T

def gram(factor):
    return jnp.dot(factor.T, factor, precision=lax.Precision.HIGHEST)

def reference(tensor, factor_two, factor_three, factor_four):
    khatri = (factor_four[:, None, :] * factor_three[None, :, :]).reshape(FOURTH * DIM_THREE, RANK).astype(jnp.bfloat16)
    flat = tensor.reshape(DIM_ONE, DIM_TWO, FOURTH * DIM_THREE)
    root = lax.map(lambda slab: jnp.dot(slab.astype(jnp.float32), khatri.astype(jnp.float32), preferred_element_type=jnp.float32), flat)
    gram_two = gram(factor_two)
    gram_three = gram(factor_three)
    gram_four = gram(factor_four)
    mode_one = jnp.einsum('abr,br->ar', root, factor_two, precision=lax.Precision.HIGHEST)
    new_one = solve_rows(mode_one, gram_two * gram_three * gram_four)
    gram_one = gram(new_one)
    mode_two = jnp.einsum('abr,ar->br', root, new_one, precision=lax.Precision.HIGHEST)
    new_two = solve_rows(mode_two, gram_one * gram_three * gram_four)
    return (new_one, new_two)
```

```python
import functools

import jax
import jax.numpy as jnp
from jax import lax
from jax.experimental import pallas as pl
from jax.experimental.pallas import tpu as pltpu
from jax.sharding import PartitionSpec as P

MESH = pl.DeviceIdType.MESH
LANES = 128
SUBLANES = 8
EXACT = lax.Precision.HIGHEST


def dot_exact(left, right):
    return jnp.dot(left, right, precision=EXACT, preferred_element_type=jnp.float32)


def iota(shape, dim):
    return lax.broadcasted_iota(jnp.int32, shape, dim)


def spread(value, rank):
    return jnp.concatenate([value] * (LANES // rank), axis=1)


def pack(wide, rank):
    groups = LANES // rank
    rows = wide.shape[0] // groups
    group = iota((rows, LANES), 1) // rank
    packed = wide[:rows]
    for g in range(1, groups):
        packed = jnp.where(group == g, wide[g * rows:(g + 1) * rows], packed)
    return packed


def unpack_masked(packed, rank):
    group = iota(packed.shape, 1) // rank
    return jnp.concatenate(
        [jnp.where(group == g, packed, 0.0) for g in range(LANES // rank)], axis=0
    )


def inverse_wide(system_packed, rank):
    full = unpack_masked(system_packed, rank)
    shift = LANES // 2
    while shift >= rank:
        full = full + pltpu.roll(full, shift, 1)
        shift //= 2
    lane = iota((rank, LANES), 1)
    row = iota((rank, LANES), 0)
    work = jnp.where(lane < rank, full, jnp.where(lane % rank == row, 1.0, 0.0))
    for k in range(0, rank, 2):
        row_a, row_b = work[k:k + 1, :], work[k + 1:k + 2, :]
        col_a, col_b = work[:, k:k + 1], work[:, k + 1:k + 2]
        aa, ab = row_a[:, k:k + 1], row_a[:, k + 1:k + 2]
        ba, bb = row_b[:, k:k + 1], row_b[:, k + 1:k + 2]
        inv_a = 1.0 / aa
        ratio = ab * inv_a
        inv_b = 1.0 / (bb - ba * ratio)
        first = row_a * inv_a
        second = (row_b - ba * first) * inv_b
        first = first - ratio * second
        work = jnp.where(
            row == k, first, jnp.where(row == k + 1, second, work - col_a * first - col_b * second)
        )
    return jnp.where(lane < rank, pltpu.roll(work, rank, 1), work)


def kernel(
    sizes, chunks,
    tensor_hbm, two_hbm, three_hbm, four_hbm,
    one_out, two_out,
    slab, two_ref, three_ref, four_ref, root_ref, fold_ref,
    gram_two_slots, gram_three_slots, gram_one_slots, ka_slots, ja_slots, mix_slots,
    load_sems, small_sems,
    gram_two_send, gram_two_recv, gram_three_send, gram_three_recv,
    gram_one_send, gram_one_recv, ka_send, ka_recv, ja_send, ja_recv, mix_send, mix_recv,
):
    n_ia, n_ja, n_ka, rows_first, rows_second, fourth_len, rank = sizes
    halves = LANES // (fourth_len * rank)
    depth = rows_second * fourth_len
    half_first = rows_first // halves
    half_rows = half_first * depth
    per_chunk = half_first // chunks
    chunk_rows = per_chunk * depth
    my_ia, my_ja, my_ka = lax.axis_index("ia"), lax.axis_index("ja"), lax.axis_index("ka")

    small = [
        pltpu.make_async_copy(src, dst, small_sems.at[n])
        for n, (src, dst) in enumerate(
            ((two_hbm, two_ref), (three_hbm, three_ref), (four_hbm, four_ref))
        )
    ]
    for copy in small:
        copy.start()
    loads = []
    for c in range(chunks):
        for h in range(halves):
            part = pl.ds(h * half_rows + c * chunk_rows, chunk_rows)
            copy = pltpu.make_async_copy(
                tensor_hbm.at[part], slab.at[part], load_sems.at[c * halves + h]
            )
            copy.start()
            loads.append(copy)

    def mix_peer(d):
        place = lax.rem(my_ia * n_ka + my_ka + d, n_ia * n_ka)
        return place // n_ka, lax.rem(place, n_ka)

    barrier = pltpu.get_barrier_semaphore()
    for d in range(1, n_ja):
        pl.semaphore_signal(
            barrier, inc=1, device_id={"ja": lax.rem(my_ja + d, n_ja)}, device_id_type=MESH
        )
    for d in range(1, n_ia * n_ka):
        ia, ka = mix_peer(d)
        pl.semaphore_signal(
            barrier, inc=1, device_id={"ia": ia, "ka": ka}, device_id_type=MESH
        )

    def exchange(slots, send_sems, recv_sems, axis, me, count):
        copies = []
        for d in range(1, count):
            copy = pltpu.make_async_remote_copy(
                src_ref=slots.at[me], dst_ref=slots.at[me],
                send_sem=send_sems.at[d - 1], recv_sem=recv_sems.at[me],
                device_id={axis: lax.rem(me + d, count)}, device_id_type=MESH,
            )
            copy.start()
            copies.append(copy)
        return copies

    def gather(slots, send_sems, recv_sems, me, count):
        for d in range(1, count):
            source = lax.rem(me + d, count)
            pltpu.make_async_remote_copy(
                src_ref=slots.at[source], dst_ref=slots.at[source],
                send_sem=send_sems.at[d - 1], recv_sem=recv_sems.at[source],
                device_id={"ja": my_ja}, device_id_type=MESH,
            ).wait_recv()
        total = slots[0]
        for s in range(1, count):
            total = total + slots[s]
        return total

    for copy in small:
        copy.wait()
    two = spread(two_ref[...], rank)
    three = spread(three_ref[...], rank)
    four = four_ref[...]
    gram_two_slots[my_ja] = pack(dot_exact(two.T, two)[:rank], rank)
    gram_three_slots[my_ka] = pack(dot_exact(three.T, three)[:rank], rank)

    pl.semaphore_wait(barrier, n_ja - 1 + n_ia * n_ka - 1)
    pending = exchange(gram_two_slots, gram_two_send, gram_two_recv, "ja", my_ja, n_ja)
    pending += exchange(gram_three_slots, gram_three_send, gram_three_recv, "ka", my_ka, n_ka)

    four_wide = jnp.concatenate([four[l:l + 1] for l in range(fourth_len)] * halves, axis=1)
    khatri = three * four_wide
    lane_half = iota(khatri.shape, 1) // (fourth_len * rank)
    weights = jnp.concatenate(
        [jnp.where(lane_half == h, khatri, 0.0).astype(jnp.bfloat16) for h in range(halves)], axis=0
    )
    row_of = iota((depth, rows_second), 0) // fourth_len
    repeat_rows = jnp.where(row_of == iota((depth, rows_second), 1), 1.0, 0.0)
    lane_fourth = lax.rem(iota((depth, LANES), 1) // rank, fourth_len)
    own_fourth = lane_fourth == lax.rem(iota((depth, LANES), 0), fourth_len)
    scaled = jnp.where(own_fourth, dot_exact(repeat_rows, two), 0.0)

    sums = []
    for c in range(chunks):
        for h in range(halves):
            loads[c * halves + h].wait()
        left = jnp.concatenate(
            [slab[pl.ds(h * half_rows + c * chunk_rows, chunk_rows), :] for h in range(halves)], axis=1
        )
        block = jnp.dot(left, weights, preferred_element_type=jnp.float32)
        root_ref[pl.ds(c * chunk_rows, chunk_rows), :] = block
        for i in range(per_chunk):
            term = block[i * depth:(i + 1) * depth] * scaled
            sums.append(jnp.sum(term, axis=0, keepdims=True))
    mode = jnp.concatenate(sums, axis=0)
    step = rank
    lane = iota(mode.shape, 1)
    folded = mode
    for l in range(1, fourth_len):
        folded = folded + jnp.where(
            lax.rem(lane, fourth_len * rank) < (fourth_len - l) * rank,
            pltpu.roll(mode, LANES - l * rank, 1),
            pltpu.roll(mode, (fourth_len - l) * rank, 1),
        )
    sub_rows = half_first // fourth_len
    sub = lax.rem(iota((sub_rows, LANES), 1) // rank, fourth_len)
    packed = folded[:sub_rows]
    for l in range(1, fourth_len):
        packed = jnp.where(sub == l, folded[l * sub_rows:(l + 1) * sub_rows], packed)
    ka_slots[my_ka] = packed
    pending += exchange(ka_slots, ka_send, ka_recv, "ka", my_ka, n_ka)

    gram_three = gather(gram_three_slots, gram_three_send, gram_three_recv, my_ka, n_ka)
    own_four = pack(
        sum(four[l:l + 1].T * spread(four[l:l + 1], rank) for l in range(fourth_len)), rank
    )
    gram_fixed = gram_three * own_four

    ja_slots[my_ja] = gather(ka_slots, ka_send, ka_recv, my_ka, n_ka)
    pending += exchange(ja_slots, ja_send, ja_recv, "ja", my_ja, n_ja)

    gram_two = gather(gram_two_slots, gram_two_send, gram_two_recv, my_ja, n_ja)
    inv = inverse_wide(gram_two * gram_fixed, rank)
    inv = jnp.concatenate([inv] * (LANES // rank), axis=0)

    total = gather(ja_slots, ja_send, ja_recv, my_ja, n_ja)
    new_one = dot_exact(unpack_masked(total, rank), inv)
    gram_one_slots[my_ia] = pack(dot_exact(new_one.T, new_one)[:rank], rank)
    pending += exchange(gram_one_slots, gram_one_send, gram_one_recv, "ia", my_ia, n_ia)
    one_out[...] = new_one[:, :rank]

    half_of = iota((half_first, LANES), 1) // (fourth_len * rank)
    spread_one = new_one[:half_first]
    for h in range(1, halves):
        spread_one = jnp.where(half_of == h, new_one[h * half_first:(h + 1) * half_first], spread_one)
    acc = jnp.zeros((depth, LANES), jnp.float32)
    for i in range(half_first):
        acc = acc + root_ref[pl.ds(i * depth, depth), :] * spread_one[i:i + 1]
    acc = jnp.where(own_fourth, acc, 0.0)
    shift = LANES // 2
    while shift >= rank:
        acc = acc + pltpu.roll(acc, shift, 1)
        shift //= 2
    fold_ref[...] = acc
    mode_two = fold_ref[pl.ds(0, rows_second, fourth_len), :]
    for l in range(1, fourth_len):
        mode_two = mode_two + fold_ref[pl.ds(l, rows_second, fourth_len), :]
    my_mix = my_ia * n_ka + my_ka
    mix_slots[my_mix] = pack(mode_two, rank)
    for d in range(1, n_ia * n_ka):
        ia, ka = mix_peer(d)
        copy = pltpu.make_async_remote_copy(
            src_ref=mix_slots.at[my_mix], dst_ref=mix_slots.at[my_mix],
            send_sem=mix_send.at[d - 1], recv_sem=mix_recv.at[my_mix],
            device_id={"ia": ia, "ka": ka}, device_id_type=MESH,
        )
        copy.start()
        pending.append(copy)

    gram_one = gather(gram_one_slots, gram_one_send, gram_one_recv, my_ia, n_ia)
    inv = inverse_wide(gram_one * gram_fixed, rank)
    inv = jnp.concatenate([inv] * (LANES // rank), axis=0)
    total = gather(mix_slots, mix_send, mix_recv, my_mix, n_ia * n_ka)
    two_out[...] = dot_exact(unpack_masked(total, rank), inv)[:, :rank]

    for copy in pending:
        copy.wait_send()


def per_device(n_ia, n_ja, n_ka, tensor, factor_two, factor_three, factor_four):
    rows_first, rows_second, fourth_len, rows_third = tensor.shape
    rank = factor_two.shape[1]
    halves = LANES // (fourth_len * rank)
    depth = rows_second * fourth_len
    chunks = 4
    sizes = (n_ia, n_ja, n_ka, rows_first, rows_second, fourth_len, rank)
    gram_rows = rank * rank // LANES
    one_rows = rows_first * rank // LANES
    two_rows = rows_second * rank // LANES
    n_mix = n_ia * n_ka
    dma = pltpu.SemaphoreType.DMA

    def pair(count):
        return [dma((max(count - 1, 1),)), dma((count,))]

    f32 = jnp.float32
    return pl.pallas_call(
        functools.partial(kernel, sizes, chunks),
        out_shape=(
            jax.ShapeDtypeStruct((rows_first, rank), f32),
            jax.ShapeDtypeStruct((rows_second, rank), f32),
        ),
        in_specs=[pl.BlockSpec(memory_space=pl.ANY)] * 4,
        out_specs=(pl.BlockSpec(memory_space=pltpu.VMEM),) * 2,
        scratch_shapes=[
            pltpu.VMEM((rows_first * depth, rows_third), jnp.bfloat16),
            pltpu.VMEM(factor_two.shape, f32),
            pltpu.VMEM(factor_three.shape, f32),
            pltpu.VMEM(factor_four.shape, f32),
            pltpu.VMEM((rows_first * depth // halves, LANES), f32),
            pltpu.VMEM((depth, LANES), f32),
            pltpu.VMEM((n_ja, gram_rows, LANES), f32),
            pltpu.VMEM((n_ka, gram_rows, LANES), f32),
            pltpu.VMEM((n_ia, gram_rows, LANES), f32),
            pltpu.VMEM((n_ka, one_rows, LANES), f32),
            pltpu.VMEM((n_ja, one_rows, LANES), f32),
            pltpu.VMEM((n_mix, two_rows, LANES), f32),
            dma((chunks * halves,)),
            dma((3,)),
            *pair(n_ja), *pair(n_ka), *pair(n_ia), *pair(n_ka), *pair(n_ja), *pair(n_mix),
        ],
        compiler_params=pltpu.CompilerParams(collective_id=0, has_side_effects=True),
        name="als_sweep",
    )(
        tensor.reshape(rows_first * depth, rows_third), factor_two, factor_three, factor_four
    )


def solution(mesh):
    return jax.shard_map(
        functools.partial(per_device, mesh.shape["ia"], mesh.shape["ja"], mesh.shape["ka"]),
        mesh=mesh,
        in_specs=(P("ia", "ja", None, "ka"), P("ja", None), P("ka", None), P()),
        out_specs=(P("ia", None), P("ja", None)),
        check_vma=False,
    )
```

```python
import functools

import jax
import jax.numpy as jnp
from jax import lax
from jax.experimental import pallas as pl
from jax.experimental.pallas import tpu as pltpu
from jax.sharding import PartitionSpec as P

MESH = pl.DeviceIdType.MESH
LANES = 128
SUBLANES = 8
EXACT = lax.Precision.HIGHEST


def dot_exact(left, right):
    return jnp.dot(left, right, precision=EXACT, preferred_element_type=jnp.float32)


def iota(shape, dim):
    return lax.broadcasted_iota(jnp.int32, shape, dim)


def spread(value, rank):
    return jnp.concatenate([value] * (LANES // rank), axis=1)


def pack(wide, rank):
    groups = LANES // rank
    rows = wide.shape[0] // groups
    group = iota((rows, LANES), 1) // rank
    packed = wide[:rows]
    for g in range(1, groups):
        packed = jnp.where(group == g, wide[g * rows:(g + 1) * rows], packed)
    return packed


def unpack_masked(packed, rank):
    group = iota(packed.shape, 1) // rank
    return jnp.concatenate(
        [jnp.where(group == g, packed, 0.0) for g in range(LANES // rank)], axis=0
    )


def inverse_wide(system_packed, rank):
    full = unpack_masked(system_packed, rank)
    shift = LANES // 2
    while shift >= rank:
        full = full + pltpu.roll(full, shift, 1)
        shift //= 2
    lane = iota((rank, LANES), 1)
    row = iota((rank, LANES), 0)
    work = jnp.where(lane < rank, full, jnp.where(lane % rank == row, 1.0, 0.0))
    for k in range(0, rank, 2):
        row_a, row_b = work[k:k + 1, :], work[k + 1:k + 2, :]
        col_a, col_b = work[:, k:k + 1], work[:, k + 1:k + 2]
        aa, ab = row_a[:, k:k + 1], row_a[:, k + 1:k + 2]
        ba, bb = row_b[:, k:k + 1], row_b[:, k + 1:k + 2]
        inv_a = 1.0 / aa
        ratio = ab * inv_a
        inv_b = 1.0 / (bb - ba * ratio)
        first = row_a * inv_a
        second = (row_b - ba * first) * inv_b
        first = first - ratio * second
        work = jnp.where(
            row == k, first, jnp.where(row == k + 1, second, work - col_a * first - col_b * second)
        )
    return jnp.where(lane < rank, pltpu.roll(work, rank, 1), work)


def kernel(
    sizes, chunks,
    tensor_hbm, two_hbm, three_hbm, four_hbm,
    one_out, two_out,
    slab, two_ref, three_ref, four_ref, root_ref, fold_ref,
    gram_two_slots, gram_three_slots, gram_one_slots, ka_slots, ja_slots, mix_slots,
    load_sems, small_sems,
    gram_two_send, gram_two_recv, gram_three_send, gram_three_recv,
    gram_one_send, gram_one_recv, ka_send, ka_recv, ja_send, ja_recv, mix_send, mix_recv,
):
    n_ia, n_ja, n_ka, rows_first, rows_second, fourth_len, rank = sizes
    halves = LANES // (fourth_len * rank)
    depth = rows_second * fourth_len
    half_first = rows_first // halves
    half_rows = half_first * depth
    per_chunk = half_first // chunks
    chunk_rows = per_chunk * depth
    my_ia, my_ja, my_ka = lax.axis_index("ia"), lax.axis_index("ja"), lax.axis_index("ka")

    small = [
        pltpu.make_async_copy(src, dst, small_sems.at[n])
        for n, (src, dst) in enumerate(
            ((two_hbm, two_ref), (three_hbm, three_ref), (four_hbm, four_ref))
        )
    ]
    for copy in small:
        copy.start()
    loads = []
    for c in range(chunks):
        for h in range(halves):
            part = pl.ds(h * half_rows + c * chunk_rows, chunk_rows)
            copy = pltpu.make_async_copy(
                tensor_hbm.at[part], slab.at[part], load_sems.at[c * halves + h]
            )
            copy.start()
            loads.append(copy)

    def mix_peer(d):
        place = lax.rem(my_ia * n_ka + my_ka + d, n_ia * n_ka)
        return place // n_ka, lax.rem(place, n_ka)

    barrier = pltpu.get_barrier_semaphore()
    for d in range(1, n_ja):
        pl.semaphore_signal(
            barrier, inc=1, device_id={"ja": lax.rem(my_ja + d, n_ja)}, device_id_type=MESH
        )
    for d in range(1, n_ia * n_ka):
        ia, ka = mix_peer(d)
        pl.semaphore_signal(
            barrier, inc=1, device_id={"ia": ia, "ka": ka}, device_id_type=MESH
        )

    def exchange(slots, send_sems, recv_sems, axis, me, count):
        copies = []
        for d in range(1, count):
            copy = pltpu.make_async_remote_copy(
                src_ref=slots.at[me], dst_ref=slots.at[me],
                send_sem=send_sems.at[d - 1], recv_sem=recv_sems.at[me],
                device_id={axis: lax.rem(me + d, count)}, device_id_type=MESH,
            )
            copy.start()
            copies.append(copy)
        return copies

    def gather(slots, send_sems, recv_sems, me, count):
        for d in range(1, count):
            source = lax.rem(me + d, count)
            pltpu.make_async_remote_copy(
                src_ref=slots.at[source], dst_ref=slots.at[source],
                send_sem=send_sems.at[d - 1], recv_sem=recv_sems.at[source],
                device_id={"ja": my_ja}, device_id_type=MESH,
            ).wait_recv()
        total = slots[0]
        for s in range(1, count):
            total = total + slots[s]
        return total

    for copy in small:
        copy.wait()
    two_t, three_t = two_ref[...], three_ref[...]
    two = jnp.concatenate([two_t] * (LANES // rank), axis=0).T
    three = jnp.concatenate([three_t] * (LANES // rank), axis=0).T
    four = four_ref[...]
    gram_two_slots[my_ja] = pack(dot_exact(two_t, two), rank)
    gram_three_slots[my_ka] = pack(dot_exact(three_t, three), rank)

    pl.semaphore_wait(barrier, n_ja - 1 + n_ia * n_ka - 1)
    pending = exchange(gram_two_slots, gram_two_send, gram_two_recv, "ja", my_ja, n_ja)
    pending += exchange(gram_three_slots, gram_three_send, gram_three_recv, "ka", my_ka, n_ka)

    four_wide = jnp.concatenate([four[l:l + 1] for l in range(fourth_len)] * halves, axis=1)
    khatri = three * four_wide
    lane_half = iota(khatri.shape, 1) // (fourth_len * rank)
    weights = jnp.concatenate(
        [jnp.where(lane_half == h, khatri, 0.0).astype(jnp.bfloat16) for h in range(halves)], axis=0
    )
    row_of = iota((depth, rows_second), 0) // fourth_len
    repeat_rows = jnp.where(row_of == iota((depth, rows_second), 1), 1.0, 0.0)
    lane_fourth = lax.rem(iota((depth, LANES), 1) // rank, fourth_len)
    own_fourth = lane_fourth == lax.rem(iota((depth, LANES), 0), fourth_len)
    scaled = jnp.where(own_fourth, dot_exact(repeat_rows, two), 0.0)

    sums = []
    for c in range(chunks):
        for h in range(halves):
            loads[c * halves + h].wait()
        left = jnp.concatenate(
            [slab[pl.ds(h * half_rows + c * chunk_rows, chunk_rows), :] for h in range(halves)], axis=1
        )
        block = jnp.dot(left, weights, preferred_element_type=jnp.float32)
        root_ref[pl.ds(c * chunk_rows, chunk_rows), :] = block
        for i in range(per_chunk):
            term = block[i * depth:(i + 1) * depth] * scaled
            sums.append(jnp.sum(term, axis=0, keepdims=True))
    mode = jnp.concatenate(sums, axis=0)
    step = rank
    lane = iota(mode.shape, 1)
    folded = mode
    for l in range(1, fourth_len):
        folded = folded + jnp.where(
            lax.rem(lane, fourth_len * rank) < (fourth_len - l) * rank,
            pltpu.roll(mode, LANES - l * rank, 1),
            pltpu.roll(mode, (fourth_len - l) * rank, 1),
        )
    sub_rows = half_first // fourth_len
    sub = lax.rem(iota((sub_rows, LANES), 1) // rank, fourth_len)
    packed = folded[:sub_rows]
    for l in range(1, fourth_len):
        packed = jnp.where(sub == l, folded[l * sub_rows:(l + 1) * sub_rows], packed)
    ka_slots[my_ka] = packed
    pending += exchange(ka_slots, ka_send, ka_recv, "ka", my_ka, n_ka)

    gram_three = gather(gram_three_slots, gram_three_send, gram_three_recv, my_ka, n_ka)
    own_four = pack(
        sum(four[l:l + 1].T * spread(four[l:l + 1], rank) for l in range(fourth_len)), rank
    )
    gram_fixed = gram_three * own_four

    ja_slots[my_ja] = gather(ka_slots, ka_send, ka_recv, my_ka, n_ka)
    pending += exchange(ja_slots, ja_send, ja_recv, "ja", my_ja, n_ja)

    gram_two = gather(gram_two_slots, gram_two_send, gram_two_recv, my_ja, n_ja)
    inv = inverse_wide(gram_two * gram_fixed, rank)
    inv = jnp.concatenate([inv] * (LANES // rank), axis=0)

    total = gather(ja_slots, ja_send, ja_recv, my_ja, n_ja)
    new_one = dot_exact(unpack_masked(total, rank), inv)
    new_one_t = new_one.T[:rank]
    gram_one_slots[my_ia] = pack(dot_exact(new_one_t, new_one), rank)
    pending += exchange(gram_one_slots, gram_one_send, gram_one_recv, "ia", my_ia, n_ia)
    one_out[...] = new_one_t

    half_of = iota((half_first, LANES), 1) // (fourth_len * rank)
    spread_one = new_one[:half_first]
    for h in range(1, halves):
        spread_one = jnp.where(half_of == h, new_one[h * half_first:(h + 1) * half_first], spread_one)
    acc = jnp.zeros((depth, LANES), jnp.float32)
    for i in range(half_first):
        acc = acc + root_ref[pl.ds(i * depth, depth), :] * spread_one[i:i + 1]
    acc = jnp.where(own_fourth, acc, 0.0)
    shift = LANES // 2
    while shift >= rank:
        acc = acc + pltpu.roll(acc, shift, 1)
        shift //= 2
    fold_ref[...] = acc
    mode_two = fold_ref[pl.ds(0, rows_second, fourth_len), :]
    for l in range(1, fourth_len):
        mode_two = mode_two + fold_ref[pl.ds(l, rows_second, fourth_len), :]
    my_mix = my_ia * n_ka + my_ka
    mix_slots[my_mix] = pack(mode_two, rank)
    for d in range(1, n_ia * n_ka):
        ia, ka = mix_peer(d)
        copy = pltpu.make_async_remote_copy(
            src_ref=mix_slots.at[my_mix], dst_ref=mix_slots.at[my_mix],
            send_sem=mix_send.at[d - 1], recv_sem=mix_recv.at[my_mix],
            device_id={"ia": ia, "ka": ka}, device_id_type=MESH,
        )
        copy.start()
        pending.append(copy)

    gram_one = gather(gram_one_slots, gram_one_send, gram_one_recv, my_ia, n_ia)
    inv = inverse_wide(gram_one * gram_fixed, rank)
    total = gather(mix_slots, mix_send, mix_recv, my_mix, n_ia * n_ka)
    two_out[...] = lax.dot_general(
        inv, unpack_masked(total, rank), (((1,), (1,)), ((), ())),
        precision=EXACT, preferred_element_type=jnp.float32,
    )

    for copy in pending:
        copy.wait_send()


def per_device(n_ia, n_ja, n_ka, tensor, factor_two, factor_three, factor_four):
    rows_first, rows_second, fourth_len, rows_third = tensor.shape
    rank = factor_two.shape[1]
    halves = LANES // (fourth_len * rank)
    depth = rows_second * fourth_len
    chunks = 4
    sizes = (n_ia, n_ja, n_ka, rows_first, rows_second, fourth_len, rank)
    gram_rows = rank * rank // LANES
    one_rows = rows_first * rank // LANES
    two_rows = rows_second * rank // LANES
    n_mix = n_ia * n_ka
    dma = pltpu.SemaphoreType.DMA

    def pair(count):
        return [dma((max(count - 1, 1),)), dma((count,))]

    f32 = jnp.float32
    one_t, two_t = pl.pallas_call(
        functools.partial(kernel, sizes, chunks),
        out_shape=(
            jax.ShapeDtypeStruct((rank, rows_first), f32),
            jax.ShapeDtypeStruct((rank, rows_second), f32),
        ),
        in_specs=[pl.BlockSpec(memory_space=pl.ANY)] * 4,
        out_specs=(pl.BlockSpec(memory_space=pltpu.VMEM),) * 2,
        scratch_shapes=[
            pltpu.VMEM((rows_first * depth, rows_third), jnp.bfloat16),
            pltpu.VMEM(factor_two.shape[::-1], f32),
            pltpu.VMEM(factor_three.shape[::-1], f32),
            pltpu.VMEM(factor_four.shape, f32),
            pltpu.VMEM((rows_first * depth // halves, LANES), f32),
            pltpu.VMEM((depth, LANES), f32),
            pltpu.VMEM((n_ja, gram_rows, LANES), f32),
            pltpu.VMEM((n_ka, gram_rows, LANES), f32),
            pltpu.VMEM((n_ia, gram_rows, LANES), f32),
            pltpu.VMEM((n_ka, one_rows, LANES), f32),
            pltpu.VMEM((n_ja, one_rows, LANES), f32),
            pltpu.VMEM((n_mix, two_rows, LANES), f32),
            dma((chunks * halves,)),
            dma((3,)),
            *pair(n_ja), *pair(n_ka), *pair(n_ia), *pair(n_ka), *pair(n_ja), *pair(n_mix),
        ],
        compiler_params=pltpu.CompilerParams(collective_id=0, has_side_effects=True),
        name="als_sweep",
    )(
        tensor.reshape(rows_first * depth, rows_third), factor_two.T, factor_three.T, factor_four
    )
    return one_t.T, two_t.T


def solution(mesh):
    return jax.shard_map(
        functools.partial(per_device, mesh.shape["ia"], mesh.shape["ja"], mesh.shape["ka"]),
        mesh=mesh,
        in_specs=(P("ia", "ja", None, "ka"), P("ja", None), P("ka", None), P()),
        out_specs=(P("ia", None), P("ja", None)),
        check_vma=False,
    )
```

```python
import functools

import jax
import jax.numpy as jnp
from jax import lax
from jax.experimental import pallas as pl
from jax.experimental.pallas import tpu as pltpu
from jax.sharding import PartitionSpec as P

MESH = pl.DeviceIdType.MESH
LANES = 128
SUBLANES = 8
EXACT = lax.Precision.HIGHEST


def dot_exact(left, right):
    return jnp.dot(left, right, precision=EXACT, preferred_element_type=jnp.float32)


def iota(shape, dim):
    return lax.broadcasted_iota(jnp.int32, shape, dim)


def spread(value, rank):
    return jnp.concatenate([value] * (LANES // rank), axis=1)


def pack(wide, rank):
    groups = LANES // rank
    rows = wide.shape[0] // groups
    group = iota((rows, LANES), 1) // rank
    packed = wide[:rows]
    for g in range(1, groups):
        packed = jnp.where(group == g, wide[g * rows:(g + 1) * rows], packed)
    return packed


def unpack_masked(packed, rank):
    group = iota(packed.shape, 1) // rank
    return jnp.concatenate(
        [jnp.where(group == g, packed, 0.0) for g in range(LANES // rank)], axis=0
    )


def inverse_wide(system_packed, rank):
    full = unpack_masked(system_packed, rank)
    shift = LANES // 2
    while shift >= rank:
        full = full + pltpu.roll(full, shift, 1)
        shift //= 2
    lane = iota((rank, LANES), 1)
    row = iota((rank, LANES), 0)
    work = jnp.where(lane < rank, full, jnp.where(lane % rank == row, 1.0, 0.0))
    blocks = [work[b:b + SUBLANES] for b in range(0, rank, SUBLANES)]
    sub = iota((SUBLANES, LANES), 0)

    def eliminate(values, column, pivot_row, place):
        out = [v - c * pivot_row for v, c in zip(values, column)]
        home = place // SUBLANES
        out[home] = jnp.where(sub == place % SUBLANES, pivot_row, out[home])
        return out

    def row_of(values, place):
        at = place % SUBLANES
        return values[place // SUBLANES][at:at + 1]

    for start in range(0, rank, SUBLANES):
        window = [
            [jnp.broadcast_to(v[:, start + c:start + c + 1], (SUBLANES, LANES)) for v in blocks]
            for c in range(SUBLANES)
        ]
        for c in range(SUBLANES):
            place = start + c
            column = window[c]
            scale = 1.0 / row_of(column, place)
            for later in range(c + 1, SUBLANES):
                window[later] = eliminate(
                    window[later], column, row_of(window[later], place) * scale, place
                )
            blocks = eliminate(blocks, column, row_of(blocks, place) * scale, place)
    work = jnp.concatenate(blocks, axis=0)
    return jnp.where(lane < rank, pltpu.roll(work, rank, 1), work)


def kernel(
    sizes, chunks,
    tensor_hbm, two_hbm, three_hbm, four_hbm,
    one_out, two_out,
    slab, two_ref, three_ref, four_ref, root_ref, fold_ref,
    gram_two_slots, gram_three_slots, gram_one_slots, ka_slots, ja_slots, mix_slots,
    load_sems, small_sems,
    gram_two_send, gram_two_recv, gram_three_send, gram_three_recv,
    gram_one_send, gram_one_recv, ka_send, ka_recv, ja_send, ja_recv, mix_send, mix_recv,
):
    n_ia, n_ja, n_ka, rows_first, rows_second, fourth_len, rank = sizes
    halves = LANES // (fourth_len * rank)
    depth = rows_second * fourth_len
    half_first = rows_first // halves
    half_rows = half_first * depth
    per_chunk = half_first // chunks
    chunk_rows = per_chunk * depth
    my_ia, my_ja, my_ka = lax.axis_index("ia"), lax.axis_index("ja"), lax.axis_index("ka")

    small = [
        pltpu.make_async_copy(src, dst, small_sems.at[n])
        for n, (src, dst) in enumerate(
            ((two_hbm, two_ref), (three_hbm, three_ref), (four_hbm, four_ref))
        )
    ]
    for copy in small:
        copy.start()
    loads = []
    for c in range(chunks):
        for h in range(halves):
            part = pl.ds(h * half_rows + c * chunk_rows, chunk_rows)
            copy = pltpu.make_async_copy(
                tensor_hbm.at[part], slab.at[part], load_sems.at[c * halves + h]
            )
            copy.start()
            loads.append(copy)

    def mix_peer(d):
        place = lax.rem(my_ia * n_ka + my_ka + d, n_ia * n_ka)
        return place // n_ka, lax.rem(place, n_ka)

    barrier = pltpu.get_barrier_semaphore()
    for d in range(1, n_ja):
        pl.semaphore_signal(
            barrier, inc=1, device_id={"ja": lax.rem(my_ja + d, n_ja)}, device_id_type=MESH
        )
    for d in range(1, n_ia * n_ka):
        ia, ka = mix_peer(d)
        pl.semaphore_signal(
            barrier, inc=1, device_id={"ia": ia, "ka": ka}, device_id_type=MESH
        )

    def exchange(slots, send_sems, recv_sems, axis, me, count):
        copies = []
        for d in range(1, count):
            copy = pltpu.make_async_remote_copy(
                src_ref=slots.at[me], dst_ref=slots.at[me],
                send_sem=send_sems.at[d - 1], recv_sem=recv_sems.at[me],
                device_id={axis: lax.rem(me + d, count)}, device_id_type=MESH,
            )
            copy.start()
            copies.append(copy)
        return copies

    def gather(slots, send_sems, recv_sems, me, count):
        for d in range(1, count):
            source = lax.rem(me + d, count)
            pltpu.make_async_remote_copy(
                src_ref=slots.at[source], dst_ref=slots.at[source],
                send_sem=send_sems.at[d - 1], recv_sem=recv_sems.at[source],
                device_id={"ja": my_ja}, device_id_type=MESH,
            ).wait_recv()
        total = slots[0]
        for s in range(1, count):
            total = total + slots[s]
        return total

    for copy in small:
        copy.wait()
    two_t, three_t = two_ref[...], three_ref[...]
    two = jnp.concatenate([two_t] * (LANES // rank), axis=0).T
    three = jnp.concatenate([three_t] * (LANES // rank), axis=0).T
    four = four_ref[...]
    gram_two_slots[my_ja] = pack(dot_exact(two_t, two), rank)
    gram_three_slots[my_ka] = pack(dot_exact(three_t, three), rank)

    pl.semaphore_wait(barrier, n_ja - 1 + n_ia * n_ka - 1)
    pending = exchange(gram_two_slots, gram_two_send, gram_two_recv, "ja", my_ja, n_ja)
    pending += exchange(gram_three_slots, gram_three_send, gram_three_recv, "ka", my_ka, n_ka)

    four_wide = jnp.concatenate([four[l:l + 1] for l in range(fourth_len)] * halves, axis=1)
    khatri = three * four_wide
    lane_half = iota(khatri.shape, 1) // (fourth_len * rank)
    weights = jnp.concatenate(
        [jnp.where(lane_half == h, khatri, 0.0).astype(jnp.bfloat16) for h in range(halves)], axis=0
    )
    row_of = iota((depth, rows_second), 0) // fourth_len
    repeat_rows = jnp.where(row_of == iota((depth, rows_second), 1), 1.0, 0.0)
    lane_fourth = lax.rem(iota((depth, LANES), 1) // rank, fourth_len)
    own_fourth = lane_fourth == lax.rem(iota((depth, LANES), 0), fourth_len)
    scaled = jnp.where(own_fourth, dot_exact(repeat_rows, two), 0.0)

    sums = []
    for c in range(chunks):
        for h in range(halves):
            loads[c * halves + h].wait()
        left = jnp.concatenate(
            [slab[pl.ds(h * half_rows + c * chunk_rows, chunk_rows), :] for h in range(halves)], axis=1
        )
        block = jnp.dot(left, weights, preferred_element_type=jnp.float32)
        root_ref[pl.ds(c * chunk_rows, chunk_rows), :] = block
        for i in range(per_chunk):
            term = block[i * depth:(i + 1) * depth] * scaled
            sums.append(jnp.sum(term, axis=0, keepdims=True))
    mode = jnp.concatenate(sums, axis=0)
    step = rank
    lane = iota(mode.shape, 1)
    folded = mode
    for l in range(1, fourth_len):
        folded = folded + jnp.where(
            lax.rem(lane, fourth_len * rank) < (fourth_len - l) * rank,
            pltpu.roll(mode, LANES - l * rank, 1),
            pltpu.roll(mode, (fourth_len - l) * rank, 1),
        )
    sub_rows = half_first // fourth_len
    sub = lax.rem(iota((sub_rows, LANES), 1) // rank, fourth_len)
    packed = folded[:sub_rows]
    for l in range(1, fourth_len):
        packed = jnp.where(sub == l, folded[l * sub_rows:(l + 1) * sub_rows], packed)
    ka_slots[my_ka] = packed
    pending += exchange(ka_slots, ka_send, ka_recv, "ka", my_ka, n_ka)

    gram_three = gather(gram_three_slots, gram_three_send, gram_three_recv, my_ka, n_ka)
    own_four = pack(
        sum(four[l:l + 1].T * spread(four[l:l + 1], rank) for l in range(fourth_len)), rank
    )
    gram_fixed = gram_three * own_four

    ja_slots[my_ja] = gather(ka_slots, ka_send, ka_recv, my_ka, n_ka)
    pending += exchange(ja_slots, ja_send, ja_recv, "ja", my_ja, n_ja)

    gram_two = gather(gram_two_slots, gram_two_send, gram_two_recv, my_ja, n_ja)
    inv = inverse_wide(gram_two * gram_fixed, rank)
    inv = jnp.concatenate([inv] * (LANES // rank), axis=0)

    total = gather(ja_slots, ja_send, ja_recv, my_ja, n_ja)
    new_one = dot_exact(unpack_masked(total, rank), inv)
    new_one_t = new_one.T[:rank]
    gram_one_slots[my_ia] = pack(dot_exact(new_one_t, new_one), rank)
    pending += exchange(gram_one_slots, gram_one_send, gram_one_recv, "ia", my_ia, n_ia)
    one_out[...] = new_one_t

    half_of = iota((half_first, LANES), 1) // (fourth_len * rank)
    spread_one = new_one[:half_first]
    for h in range(1, halves):
        spread_one = jnp.where(half_of == h, new_one[h * half_first:(h + 1) * half_first], spread_one)
    acc = jnp.zeros((depth, LANES), jnp.float32)
    for i in range(half_first):
        acc = acc + root_ref[pl.ds(i * depth, depth), :] * spread_one[i:i + 1]
    acc = jnp.where(own_fourth, acc, 0.0)
    shift = LANES // 2
    while shift >= rank:
        acc = acc + pltpu.roll(acc, shift, 1)
        shift //= 2
    fold_ref[...] = acc
    mode_two = fold_ref[pl.ds(0, rows_second, fourth_len), :]
    for l in range(1, fourth_len):
        mode_two = mode_two + fold_ref[pl.ds(l, rows_second, fourth_len), :]
    my_mix = my_ia * n_ka + my_ka
    mix_slots[my_mix] = pack(mode_two, rank)
    for d in range(1, n_ia * n_ka):
        ia, ka = mix_peer(d)
        copy = pltpu.make_async_remote_copy(
            src_ref=mix_slots.at[my_mix], dst_ref=mix_slots.at[my_mix],
            send_sem=mix_send.at[d - 1], recv_sem=mix_recv.at[my_mix],
            device_id={"ia": ia, "ka": ka}, device_id_type=MESH,
        )
        copy.start()
        pending.append(copy)

    gram_one = gather(gram_one_slots, gram_one_send, gram_one_recv, my_ia, n_ia)
    inv = inverse_wide(gram_one * gram_fixed, rank)
    total = gather(mix_slots, mix_send, mix_recv, my_mix, n_ia * n_ka)
    two_out[...] = lax.dot_general(
        inv, unpack_masked(total, rank), (((1,), (1,)), ((), ())),
        precision=EXACT, preferred_element_type=jnp.float32,
    )

    for copy in pending:
        copy.wait_send()


def per_device(n_ia, n_ja, n_ka, tensor, factor_two, factor_three, factor_four):
    rows_first, rows_second, fourth_len, rows_third = tensor.shape
    rank = factor_two.shape[1]
    halves = LANES // (fourth_len * rank)
    depth = rows_second * fourth_len
    chunks = 4
    sizes = (n_ia, n_ja, n_ka, rows_first, rows_second, fourth_len, rank)
    gram_rows = rank * rank // LANES
    one_rows = rows_first * rank // LANES
    two_rows = rows_second * rank // LANES
    n_mix = n_ia * n_ka
    dma = pltpu.SemaphoreType.DMA

    def pair(count):
        return [dma((max(count - 1, 1),)), dma((count,))]

    f32 = jnp.float32
    one_t, two_t = pl.pallas_call(
        functools.partial(kernel, sizes, chunks),
        out_shape=(pltpu.VMEM((rank, rows_first), f32), pltpu.VMEM((rank, rows_second), f32)),
        in_specs=[pl.BlockSpec(memory_space=pltpu.HBM)] * 4,
        out_specs=(pl.BlockSpec(memory_space=pltpu.VMEM),) * 2,
        scratch_shapes=[
            pltpu.VMEM((rows_first * depth, rows_third), jnp.bfloat16),
            pltpu.VMEM(factor_two.shape[::-1], f32),
            pltpu.VMEM(factor_three.shape[::-1], f32),
            pltpu.VMEM(factor_four.shape, f32),
            pltpu.VMEM((rows_first * depth // halves, LANES), f32),
            pltpu.VMEM((depth, LANES), f32),
            pltpu.VMEM((n_ja, gram_rows, LANES), f32),
            pltpu.VMEM((n_ka, gram_rows, LANES), f32),
            pltpu.VMEM((n_ia, gram_rows, LANES), f32),
            pltpu.VMEM((n_ka, one_rows, LANES), f32),
            pltpu.VMEM((n_ja, one_rows, LANES), f32),
            pltpu.VMEM((n_mix, two_rows, LANES), f32),
            dma((chunks * halves,)),
            dma((3,)),
            *pair(n_ja), *pair(n_ka), *pair(n_ia), *pair(n_ka), *pair(n_ja), *pair(n_mix),
        ],
        compiler_params=pltpu.CompilerParams(collective_id=0, has_side_effects=True),
        name="als_sweep",
    )(
        tensor.reshape(rows_first * depth, rows_third), factor_two.T, factor_three.T, factor_four
    )
    def hand_on(one_ref, two_ref, one_out, two_out):
        one_out[...] = one_ref[...]
        two_out[...] = two_ref[...]

    one_t, two_t = pl.pallas_call(
        hand_on,
        out_shape=(
            jax.ShapeDtypeStruct((rank, rows_first), f32),
            jax.ShapeDtypeStruct((rank, rows_second), f32),
        ),
        in_specs=[pl.BlockSpec(memory_space=pltpu.VMEM)] * 2,
        out_specs=(pl.BlockSpec(memory_space=pltpu.VMEM),) * 2,
        compiler_params=pltpu.CompilerParams(vmem_limit_bytes=2 * 1024 * 1024),
        name="hand_on",
    )(one_t, two_t)
    return one_t.T, two_t.T


def solution(mesh):
    return jax.shard_map(
        functools.partial(per_device, mesh.shape["ia"], mesh.shape["ja"], mesh.shape["ka"]),
        mesh=mesh,
        in_specs=(P("ia", "ja", None, "ka"), P("ja", None), P("ka", None), P()),
        out_specs=(P("ia", None), P("ja", None)),
        check_vma=False,
    )
```

```python
import functools

import jax
import jax.numpy as jnp
from jax import lax
from jax.experimental import pallas as pl
from jax.experimental.pallas import tpu as pltpu
from jax.sharding import PartitionSpec as P

MESH = pl.DeviceIdType.MESH
LANES = 128
SUBLANES = 8
EXACT = lax.Precision.HIGHEST


def dot_exact(left, right):
    return jnp.dot(left, right, precision=EXACT, preferred_element_type=jnp.float32)


def iota(shape, dim):
    return lax.broadcasted_iota(jnp.int32, shape, dim)


def spread(value, rank):
    return jnp.concatenate([value] * (LANES // rank), axis=1)


def pack(wide, rank):
    groups = LANES // rank
    rows = wide.shape[0] // groups
    group = iota((rows, LANES), 1) // rank
    packed = wide[:rows]
    for g in range(1, groups):
        packed = jnp.where(group == g, wide[g * rows:(g + 1) * rows], packed)
    return packed


def unpack_masked(packed, rank):
    group = iota(packed.shape, 1) // rank
    return jnp.concatenate(
        [jnp.where(group == g, packed, 0.0) for g in range(LANES // rank)], axis=0
    )


def inverse_wide(system_packed, rank):
    full = unpack_masked(system_packed, rank)
    shift = LANES // 2
    while shift >= rank:
        full = full + pltpu.roll(full, shift, 1)
        shift //= 2
    lane = iota((rank, LANES), 1)
    row = iota((rank, LANES), 0)
    work = jnp.where(lane < rank, full, jnp.where(lane % rank == row, 1.0, 0.0))
    blocks = [work[b:b + SUBLANES] for b in range(0, rank, SUBLANES)]
    sub = iota((SUBLANES, LANES), 0)

    def eliminate(values, column, pivot_row, place):
        out = [v - c * pivot_row for v, c in zip(values, column)]
        home = place // SUBLANES
        out[home] = jnp.where(sub == place % SUBLANES, pivot_row, out[home])
        return out

    def row_of(values, place):
        at = place % SUBLANES
        return values[place // SUBLANES][at:at + 1]

    for start in range(0, rank, SUBLANES):
        window = [
            [jnp.broadcast_to(v[:, start + c:start + c + 1], (SUBLANES, LANES)) for v in blocks]
            for c in range(SUBLANES)
        ]
        for c in range(SUBLANES):
            place = start + c
            column = window[c]
            scale = 1.0 / row_of(column, place)
            for later in range(c + 1, SUBLANES):
                window[later] = eliminate(
                    window[later], column, row_of(window[later], place) * scale, place
                )
            blocks = eliminate(blocks, column, row_of(blocks, place) * scale, place)
    work = jnp.concatenate(blocks, axis=0)
    return jnp.where(lane < rank, pltpu.roll(work, rank, 1), work)


def kernel(
    sizes, chunks,
    tensor_hbm, two_hbm, three_hbm, four_hbm,
    one_out, two_out,
    slab, two_ref, three_ref, four_ref, root_ref, fold_ref,
    gram_two_slots, gram_three_slots, gram_one_slots, ka_slots, ja_slots, mix_slots,
    load_sems, small_sems,
    gram_two_send, gram_two_recv, gram_three_send, gram_three_recv,
    gram_one_send, gram_one_recv, ka_send, ka_recv, ja_send, ja_recv, mix_send, mix_recv,
):
    n_ia, n_ja, n_ka, rows_first, rows_second, fourth_len, rank = sizes
    halves = LANES // (fourth_len * rank)
    depth = rows_second * fourth_len
    half_first = rows_first // halves
    half_rows = half_first * depth
    per_chunk = half_first // chunks
    chunk_rows = per_chunk * depth
    my_ia, my_ja, my_ka = lax.axis_index("ia"), lax.axis_index("ja"), lax.axis_index("ka")

    small = [
        pltpu.make_async_copy(src, dst, small_sems.at[n])
        for n, (src, dst) in enumerate(
            ((two_hbm, two_ref), (three_hbm, three_ref), (four_hbm, four_ref))
        )
    ]
    for copy in small:
        copy.start()
    loads = []
    for c in range(chunks):
        for h in range(halves):
            part = pl.ds(h * half_rows + c * chunk_rows, chunk_rows)
            copy = pltpu.make_async_copy(
                tensor_hbm.at[part], slab.at[part], load_sems.at[c * halves + h]
            )
            copy.start()
            loads.append(copy)

    def mix_peer(d):
        place = lax.rem(my_ia * n_ka + my_ka + d, n_ia * n_ka)
        return place // n_ka, lax.rem(place, n_ka)

    barrier = pltpu.get_barrier_semaphore()
    for d in range(1, n_ja):
        pl.semaphore_signal(
            barrier, inc=1, device_id={"ja": lax.rem(my_ja + d, n_ja)}, device_id_type=MESH
        )
    for d in range(1, n_ia * n_ka):
        ia, ka = mix_peer(d)
        pl.semaphore_signal(
            barrier, inc=1, device_id={"ia": ia, "ka": ka}, device_id_type=MESH
        )

    def exchange(slots, send_sems, recv_sems, axis, me, count):
        copies = []
        for d in range(1, count):
            copy = pltpu.make_async_remote_copy(
                src_ref=slots.at[me], dst_ref=slots.at[me],
                send_sem=send_sems.at[d - 1], recv_sem=recv_sems.at[me],
                device_id={axis: lax.rem(me + d, count)}, device_id_type=MESH,
            )
            copy.start()
            copies.append(copy)
        return copies

    def gather(slots, send_sems, recv_sems, me, count):
        for d in range(1, count):
            source = lax.rem(me + d, count)
            pltpu.make_async_remote_copy(
                src_ref=slots.at[source], dst_ref=slots.at[source],
                send_sem=send_sems.at[d - 1], recv_sem=recv_sems.at[source],
                device_id={"ja": my_ja}, device_id_type=MESH,
            ).wait_recv()
        total = slots[0]
        for s in range(1, count):
            total = total + slots[s]
        return total

    for copy in small:
        copy.wait()
    two_t, three_t = two_ref[...], three_ref[...]
    two = jnp.concatenate([two_t] * (LANES // rank), axis=0).T
    three = jnp.concatenate([three_t] * (LANES // rank), axis=0).T
    four = four_ref[...]
    gram_two_slots[my_ja] = pack(dot_exact(two_t, two), rank)
    gram_three_slots[my_ka] = pack(dot_exact(three_t, three), rank)

    pl.semaphore_wait(barrier, n_ja - 1 + n_ia * n_ka - 1)
    pending = exchange(gram_two_slots, gram_two_send, gram_two_recv, "ja", my_ja, n_ja)
    pending += exchange(gram_three_slots, gram_three_send, gram_three_recv, "ka", my_ka, n_ka)

    four_wide = jnp.concatenate([four[l:l + 1] for l in range(fourth_len)] * halves, axis=1)
    khatri = three * four_wide
    lane_half = iota(khatri.shape, 1) // (fourth_len * rank)
    weights = jnp.concatenate(
        [jnp.where(lane_half == h, khatri, 0.0).astype(jnp.bfloat16) for h in range(halves)], axis=0
    )
    row_of = iota((depth, rows_second), 0) // fourth_len
    repeat_rows = jnp.where(row_of == iota((depth, rows_second), 1), 1.0, 0.0)
    lane_fourth = lax.rem(iota((depth, LANES), 1) // rank, fourth_len)
    own_fourth = lane_fourth == lax.rem(iota((depth, LANES), 0), fourth_len)
    scaled = jnp.where(own_fourth, dot_exact(repeat_rows, two), 0.0)

    sums = []
    for c in range(chunks):
        for h in range(halves):
            loads[c * halves + h].wait()
        left = jnp.concatenate(
            [slab[pl.ds(h * half_rows + c * chunk_rows, chunk_rows), :] for h in range(halves)], axis=1
        )
        block = jnp.dot(left, weights, preferred_element_type=jnp.float32)
        root_ref[pl.ds(c * chunk_rows, chunk_rows), :] = block
        for i in range(per_chunk):
            term = block[i * depth:(i + 1) * depth] * scaled
            sums.append(jnp.sum(term, axis=0, keepdims=True))
    mode = jnp.concatenate(sums, axis=0)
    step = rank
    lane = iota(mode.shape, 1)
    folded = mode
    for l in range(1, fourth_len):
        folded = folded + jnp.where(
            lax.rem(lane, fourth_len * rank) < (fourth_len - l) * rank,
            pltpu.roll(mode, LANES - l * rank, 1),
            pltpu.roll(mode, (fourth_len - l) * rank, 1),
        )
    sub_rows = half_first // fourth_len
    sub = lax.rem(iota((sub_rows, LANES), 1) // rank, fourth_len)
    packed = folded[:sub_rows]
    for l in range(1, fourth_len):
        packed = jnp.where(sub == l, folded[l * sub_rows:(l + 1) * sub_rows], packed)
    ka_slots[my_ka] = packed
    pending += exchange(ka_slots, ka_send, ka_recv, "ka", my_ka, n_ka)

    gram_three = gather(gram_three_slots, gram_three_send, gram_three_recv, my_ka, n_ka)
    own_four = pack(
        sum(four[l:l + 1].T * spread(four[l:l + 1], rank) for l in range(fourth_len)), rank
    )
    gram_fixed = gram_three * own_four

    ja_slots[my_ja] = gather(ka_slots, ka_send, ka_recv, my_ka, n_ka)
    pending += exchange(ja_slots, ja_send, ja_recv, "ja", my_ja, n_ja)

    gram_two = gather(gram_two_slots, gram_two_send, gram_two_recv, my_ja, n_ja)
    inv = inverse_wide(gram_two * gram_fixed, rank)
    inv = jnp.concatenate([inv] * (LANES // rank), axis=0)

    total = gather(ja_slots, ja_send, ja_recv, my_ja, n_ja)
    new_one = dot_exact(unpack_masked(total, rank), inv)
    new_one_t = new_one.T[:rank]
    gram_one_slots[my_ia] = pack(dot_exact(new_one_t, new_one), rank)
    gram_copies = exchange(gram_one_slots, gram_one_send, gram_one_recv, "ia", my_ia, n_ia)
    for copy in pending:
        copy.wait_send()
    pending = gram_copies
    one_out[...] = new_one_t

    half_of = iota((half_first, LANES), 1) // (fourth_len * rank)
    spread_one = new_one[:half_first]
    for h in range(1, halves):
        spread_one = jnp.where(half_of == h, new_one[h * half_first:(h + 1) * half_first], spread_one)
    acc = jnp.zeros((depth, LANES), jnp.float32)
    for i in range(half_first):
        acc = acc + root_ref[pl.ds(i * depth, depth), :] * spread_one[i:i + 1]
    acc = jnp.where(own_fourth, acc, 0.0)
    shift = LANES // 2
    while shift >= rank:
        acc = acc + pltpu.roll(acc, shift, 1)
        shift //= 2
    fold_ref[...] = acc
    mode_two = fold_ref[pl.ds(0, rows_second, fourth_len), :]
    for l in range(1, fourth_len):
        mode_two = mode_two + fold_ref[pl.ds(l, rows_second, fourth_len), :]
    my_mix = my_ia * n_ka + my_ka
    mix_slots[my_mix] = pack(mode_two, rank)
    for d in range(1, n_ia * n_ka):
        ia, ka = mix_peer(d)
        copy = pltpu.make_async_remote_copy(
            src_ref=mix_slots.at[my_mix], dst_ref=mix_slots.at[my_mix],
            send_sem=mix_send.at[d - 1], recv_sem=mix_recv.at[my_mix],
            device_id={"ia": ia, "ka": ka}, device_id_type=MESH,
        )
        copy.start()
        pending.append(copy)

    gram_one = gather(gram_one_slots, gram_one_send, gram_one_recv, my_ia, n_ia)
    inv = inverse_wide(gram_one * gram_fixed, rank)
    total = gather(mix_slots, mix_send, mix_recv, my_mix, n_ia * n_ka)
    two_out[...] = lax.dot_general(
        inv, unpack_masked(total, rank), (((1,), (1,)), ((), ())),
        precision=EXACT, preferred_element_type=jnp.float32,
    )

    for copy in pending:
        copy.wait_send()


def per_device(n_ia, n_ja, n_ka, tensor, factor_two, factor_three, factor_four):
    rows_first, rows_second, fourth_len, rows_third = tensor.shape
    rank = factor_two.shape[1]
    halves = LANES // (fourth_len * rank)
    depth = rows_second * fourth_len
    chunks = 1
    sizes = (n_ia, n_ja, n_ka, rows_first, rows_second, fourth_len, rank)
    gram_rows = rank * rank // LANES
    one_rows = rows_first * rank // LANES
    two_rows = rows_second * rank // LANES
    n_mix = n_ia * n_ka
    dma = pltpu.SemaphoreType.DMA

    def pair(count):
        return [dma((max(count - 1, 1),)), dma((count,))]

    f32 = jnp.float32
    one_t, two_t = pl.pallas_call(
        functools.partial(kernel, sizes, chunks),
        out_shape=(pltpu.VMEM((rank, rows_first), f32), pltpu.VMEM((rank, rows_second), f32)),
        in_specs=[pl.BlockSpec(memory_space=pltpu.HBM)] * 4,
        out_specs=(pl.BlockSpec(memory_space=pltpu.VMEM),) * 2,
        scratch_shapes=[
            pltpu.VMEM((rows_first * depth, rows_third), jnp.bfloat16),
            pltpu.VMEM(factor_two.shape[::-1], f32),
            pltpu.VMEM(factor_three.shape[::-1], f32),
            pltpu.VMEM(factor_four.shape, f32),
            pltpu.VMEM((rows_first * depth // halves, LANES), f32),
            pltpu.VMEM((depth, LANES), f32),
            pltpu.VMEM((n_ja, gram_rows, LANES), f32),
            pltpu.VMEM((n_ka, gram_rows, LANES), f32),
            pltpu.VMEM((n_ia, gram_rows, LANES), f32),
            pltpu.VMEM((n_ka, one_rows, LANES), f32),
            pltpu.VMEM((n_ja, one_rows, LANES), f32),
            pltpu.VMEM((n_mix, two_rows, LANES), f32),
            dma((chunks * halves,)),
            dma((3,)),
            *pair(n_ja), *pair(n_ka), *pair(n_ia), *pair(n_ka), *pair(n_ja), *pair(n_mix),
        ],
        compiler_params=pltpu.CompilerParams(collective_id=0, has_side_effects=True),
        name="als_sweep",
    )(
        tensor.reshape(rows_first * depth, rows_third), factor_two.T, factor_three.T, factor_four
    )
    def hand_on(one_ref, two_ref, one_out, two_out):
        one_out[...] = one_ref[...]
        two_out[...] = two_ref[...]

    one_t, two_t = pl.pallas_call(
        hand_on,
        out_shape=(
            jax.ShapeDtypeStruct((rank, rows_first), f32),
            jax.ShapeDtypeStruct((rank, rows_second), f32),
        ),
        in_specs=[pl.BlockSpec(memory_space=pltpu.VMEM)] * 2,
        out_specs=(pl.BlockSpec(memory_space=pltpu.VMEM),) * 2,
        compiler_params=pltpu.CompilerParams(vmem_limit_bytes=2 * 1024 * 1024),
        name="hand_on",
    )(one_t, two_t)
    return one_t.T, two_t.T


def solution(mesh):
    return jax.shard_map(
        functools.partial(per_device, mesh.shape["ia"], mesh.shape["ja"], mesh.shape["ka"]),
        mesh=mesh,
        in_specs=(P("ia", "ja", None, "ka"), P("ja", None), P("ka", None), P()),
        out_specs=(P("ia", None), P("ja", None)),
        check_vma=False,
    )
```

```python
import functools

import jax
import jax.numpy as jnp
from jax import lax
from jax.experimental import pallas as pl
from jax.experimental.pallas import tpu as pltpu
from jax.sharding import PartitionSpec as P

MESH = pl.DeviceIdType.MESH
LANES = 128
SUBLANES = 8
EXACT = lax.Precision.HIGHEST


def dot_exact(left, right):
    return jnp.dot(left, right, precision=EXACT, preferred_element_type=jnp.float32)


def iota(shape, dim):
    return lax.broadcasted_iota(jnp.int32, shape, dim)


def spread(value, rank):
    return jnp.concatenate([value] * (LANES // rank), axis=1)


def pack(wide, rank):
    groups = LANES // rank
    rows = wide.shape[0] // groups
    group = iota((rows, LANES), 1) // rank
    packed = wide[:rows]
    for g in range(1, groups):
        packed = jnp.where(group == g, wide[g * rows:(g + 1) * rows], packed)
    return packed


def unpack_masked(packed, rank):
    group = iota(packed.shape, 1) // rank
    return jnp.concatenate(
        [jnp.where(group == g, packed, 0.0) for g in range(LANES // rank)], axis=0
    )


def inverse_wide(system_packed, rank):
    full = unpack_masked(system_packed, rank)
    shift = LANES // 2
    while shift >= rank:
        full = full + pltpu.roll(full, shift, 1)
        shift //= 2
    lane = iota((rank, LANES), 1)
    row = iota((rank, LANES), 0)
    work = jnp.where(lane < rank, full, jnp.where(lane % rank == row, 1.0, 0.0))
    blocks = [work[b:b + SUBLANES] for b in range(0, rank, SUBLANES)]
    sub = iota((SUBLANES, LANES), 0)

    def eliminate(values, column, pivot_row, place):
        out = [v - c * pivot_row for v, c in zip(values, column)]
        home = place // SUBLANES
        out[home] = jnp.where(sub == place % SUBLANES, pivot_row, out[home])
        return out

    def row_of(values, place):
        at = place % SUBLANES
        return values[place // SUBLANES][at:at + 1]

    span = 4

    def spread_columns(start):
        return [
            [jnp.broadcast_to(v[:, at:at + 1], (SUBLANES, LANES)) for v in blocks]
            for at in range(start, min(start + span, rank))
        ]

    window = spread_columns(0)
    for start in range(0, rank, span):
        ahead = spread_columns(start + span)
        for c in range(span):
            place = start + c
            column = window[c]
            scale = 1.0 / row_of(column, place)
            for later in range(c + 1, span):
                window[later] = eliminate(
                    window[later], column, row_of(window[later], place) * scale, place
                )
            ahead = [
                eliminate(values, column, row_of(values, place) * scale, place) for values in ahead
            ]
            blocks = eliminate(blocks, column, row_of(blocks, place) * scale, place)
        window = ahead
    work = jnp.concatenate(blocks, axis=0)
    return jnp.where(lane < rank, pltpu.roll(work, rank, 1), work)


def kernel(
    sizes, chunks,
    tensor_hbm, two_hbm, three_hbm, four_hbm,
    one_out, two_out,
    slab, two_ref, three_ref, four_ref, root_ref, fold_ref,
    gram_two_slots, gram_three_slots, gram_one_slots, ka_slots, ja_slots, mix_slots,
    load_sems, small_sems,
    gram_two_send, gram_two_recv, gram_three_send, gram_three_recv,
    gram_one_send, gram_one_recv, ka_send, ka_recv, ja_send, ja_recv, mix_send, mix_recv,
):
    n_ia, n_ja, n_ka, rows_first, rows_second, fourth_len, rank = sizes
    halves = LANES // (fourth_len * rank)
    depth = rows_second * fourth_len
    half_first = rows_first // halves
    half_rows = half_first * depth
    per_chunk = half_first // chunks
    chunk_rows = per_chunk * depth
    my_ia, my_ja, my_ka = lax.axis_index("ia"), lax.axis_index("ja"), lax.axis_index("ka")

    small = [
        pltpu.make_async_copy(src, dst, small_sems.at[n])
        for n, (src, dst) in enumerate(
            ((two_hbm, two_ref), (three_hbm, three_ref), (four_hbm, four_ref))
        )
    ]
    for copy in small:
        copy.start()
    loads = []
    for c in range(chunks):
        for h in range(halves):
            part = pl.ds(h * half_rows + c * chunk_rows, chunk_rows)
            copy = pltpu.make_async_copy(
                tensor_hbm.at[part], slab.at[part], load_sems.at[c * halves + h]
            )
            copy.start()
            loads.append(copy)

    def mix_peer(d):
        place = lax.rem(my_ia * n_ka + my_ka + d, n_ia * n_ka)
        return place // n_ka, lax.rem(place, n_ka)

    barrier = pltpu.get_barrier_semaphore()
    for d in range(1, n_ja):
        pl.semaphore_signal(
            barrier, inc=1, device_id={"ja": lax.rem(my_ja + d, n_ja)}, device_id_type=MESH
        )
    for d in range(1, n_ia * n_ka):
        ia, ka = mix_peer(d)
        pl.semaphore_signal(
            barrier, inc=1, device_id={"ia": ia, "ka": ka}, device_id_type=MESH
        )

    def exchange(slots, send_sems, recv_sems, axis, me, count):
        copies = []
        for d in range(1, count):
            copy = pltpu.make_async_remote_copy(
                src_ref=slots.at[me], dst_ref=slots.at[me],
                send_sem=send_sems.at[d - 1], recv_sem=recv_sems.at[me],
                device_id={axis: lax.rem(me + d, count)}, device_id_type=MESH,
            )
            copy.start()
            copies.append(copy)
        return copies

    def gather(slots, send_sems, recv_sems, me, count):
        for d in range(1, count):
            source = lax.rem(me + d, count)
            pltpu.make_async_remote_copy(
                src_ref=slots.at[source], dst_ref=slots.at[source],
                send_sem=send_sems.at[d - 1], recv_sem=recv_sems.at[source],
                device_id={"ja": my_ja}, device_id_type=MESH,
            ).wait_recv()
        total = slots[0]
        for s in range(1, count):
            total = total + slots[s]
        return total

    for copy in small:
        copy.wait()
    two_t, three_t = two_ref[...], three_ref[...]
    two = jnp.concatenate([two_t] * (LANES // rank), axis=0).T
    three = jnp.concatenate([three_t] * (LANES // rank), axis=0).T
    four = four_ref[...]
    gram_two_slots[my_ja] = pack(dot_exact(two_t, two), rank)
    gram_three_slots[my_ka] = pack(dot_exact(three_t, three), rank)

    pl.semaphore_wait(barrier, n_ja - 1 + n_ia * n_ka - 1)
    pending = exchange(gram_two_slots, gram_two_send, gram_two_recv, "ja", my_ja, n_ja)
    pending += exchange(gram_three_slots, gram_three_send, gram_three_recv, "ka", my_ka, n_ka)

    four_wide = jnp.concatenate([four[l:l + 1] for l in range(fourth_len)] * halves, axis=1)
    khatri = three * four_wide
    lane_half = iota(khatri.shape, 1) // (fourth_len * rank)
    weights = jnp.concatenate(
        [jnp.where(lane_half == h, khatri, 0.0).astype(jnp.bfloat16) for h in range(halves)], axis=0
    )
    row_of = iota((depth, rows_second), 0) // fourth_len
    repeat_rows = jnp.where(row_of == iota((depth, rows_second), 1), 1.0, 0.0)
    lane_fourth = lax.rem(iota((depth, LANES), 1) // rank, fourth_len)
    own_fourth = lane_fourth == lax.rem(iota((depth, LANES), 0), fourth_len)
    scaled = jnp.where(own_fourth, dot_exact(repeat_rows, two), 0.0)

    sums = []
    for c in range(chunks):
        for h in range(halves):
            loads[c * halves + h].wait()
        left = jnp.concatenate(
            [slab[pl.ds(h * half_rows + c * chunk_rows, chunk_rows), :] for h in range(halves)], axis=1
        )
        block = jnp.dot(left, weights, preferred_element_type=jnp.float32)
        root_ref[pl.ds(c * chunk_rows, chunk_rows), :] = block
        for i in range(per_chunk):
            term = block[i * depth:(i + 1) * depth] * scaled
            sums.append(jnp.sum(term, axis=0, keepdims=True))
    mode = jnp.concatenate(sums, axis=0)
    step = rank
    lane = iota(mode.shape, 1)
    folded = mode
    for l in range(1, fourth_len):
        folded = folded + jnp.where(
            lax.rem(lane, fourth_len * rank) < (fourth_len - l) * rank,
            pltpu.roll(mode, LANES - l * rank, 1),
            pltpu.roll(mode, (fourth_len - l) * rank, 1),
        )
    sub_rows = half_first // fourth_len
    sub = lax.rem(iota((sub_rows, LANES), 1) // rank, fourth_len)
    packed = folded[:sub_rows]
    for l in range(1, fourth_len):
        packed = jnp.where(sub == l, folded[l * sub_rows:(l + 1) * sub_rows], packed)
    ka_slots[my_ka] = packed
    pending += exchange(ka_slots, ka_send, ka_recv, "ka", my_ka, n_ka)

    gram_three = gather(gram_three_slots, gram_three_send, gram_three_recv, my_ka, n_ka)
    own_four = pack(
        sum(four[l:l + 1].T * spread(four[l:l + 1], rank) for l in range(fourth_len)), rank
    )
    gram_fixed = gram_three * own_four

    ja_slots[my_ja] = gather(ka_slots, ka_send, ka_recv, my_ka, n_ka)
    pending += exchange(ja_slots, ja_send, ja_recv, "ja", my_ja, n_ja)

    gram_two = gather(gram_two_slots, gram_two_send, gram_two_recv, my_ja, n_ja)
    inv = inverse_wide(gram_two * gram_fixed, rank)
    inv = jnp.concatenate([inv] * (LANES // rank), axis=0)

    total = gather(ja_slots, ja_send, ja_recv, my_ja, n_ja)
    new_one = dot_exact(unpack_masked(total, rank), inv)
    new_one_t = new_one.T[:rank]
    gram_one_slots[my_ia] = pack(dot_exact(new_one_t, new_one), rank)
    gram_copies = exchange(gram_one_slots, gram_one_send, gram_one_recv, "ia", my_ia, n_ia)
    for copy in pending:
        copy.wait_send()
    pending = gram_copies
    one_out[...] = new_one_t

    half_of = iota((half_first, LANES), 1) // (fourth_len * rank)
    spread_one = new_one[:half_first]
    for h in range(1, halves):
        spread_one = jnp.where(half_of == h, new_one[h * half_first:(h + 1) * half_first], spread_one)
    acc = jnp.zeros((depth, LANES), jnp.float32)
    for i in range(half_first):
        acc = acc + root_ref[pl.ds(i * depth, depth), :] * spread_one[i:i + 1]
    acc = jnp.where(own_fourth, acc, 0.0)
    shift = LANES // 2
    while shift >= rank:
        acc = acc + pltpu.roll(acc, shift, 1)
        shift //= 2
    fold_ref[...] = acc
    mode_two = fold_ref[pl.ds(0, rows_second, fourth_len), :]
    for l in range(1, fourth_len):
        mode_two = mode_two + fold_ref[pl.ds(l, rows_second, fourth_len), :]
    my_mix = my_ia * n_ka + my_ka
    mix_slots[my_mix] = pack(mode_two, rank)
    for d in range(1, n_ia * n_ka):
        ia, ka = mix_peer(d)
        copy = pltpu.make_async_remote_copy(
            src_ref=mix_slots.at[my_mix], dst_ref=mix_slots.at[my_mix],
            send_sem=mix_send.at[d - 1], recv_sem=mix_recv.at[my_mix],
            device_id={"ia": ia, "ka": ka}, device_id_type=MESH,
        )
        copy.start()
        pending.append(copy)

    gram_one = gather(gram_one_slots, gram_one_send, gram_one_recv, my_ia, n_ia)
    inv = inverse_wide(gram_one * gram_fixed, rank)
    total = gather(mix_slots, mix_send, mix_recv, my_mix, n_ia * n_ka)
    two_out[...] = lax.dot_general(
        inv, unpack_masked(total, rank), (((1,), (1,)), ((), ())),
        precision=EXACT, preferred_element_type=jnp.float32,
    )

    for copy in pending:
        copy.wait_send()


def per_device(n_ia, n_ja, n_ka, tensor, factor_two, factor_three, factor_four):
    rows_first, rows_second, fourth_len, rows_third = tensor.shape
    rank = factor_two.shape[1]
    halves = LANES // (fourth_len * rank)
    depth = rows_second * fourth_len
    chunks = 1
    sizes = (n_ia, n_ja, n_ka, rows_first, rows_second, fourth_len, rank)
    gram_rows = rank * rank // LANES
    one_rows = rows_first * rank // LANES
    two_rows = rows_second * rank // LANES
    n_mix = n_ia * n_ka
    dma = pltpu.SemaphoreType.DMA

    def pair(count):
        return [dma((max(count - 1, 1),)), dma((count,))]

    f32 = jnp.float32
    one_t, two_t = pl.pallas_call(
        functools.partial(kernel, sizes, chunks),
        out_shape=(pltpu.VMEM((rank, rows_first), f32), pltpu.VMEM((rank, rows_second), f32)),
        in_specs=[pl.BlockSpec(memory_space=pltpu.HBM)] * 4,
        out_specs=(pl.BlockSpec(memory_space=pltpu.VMEM),) * 2,
        scratch_shapes=[
            pltpu.VMEM((rows_first * depth, rows_third), jnp.bfloat16),
            pltpu.VMEM(factor_two.shape[::-1], f32),
            pltpu.VMEM(factor_three.shape[::-1], f32),
            pltpu.VMEM(factor_four.shape, f32),
            pltpu.VMEM((rows_first * depth // halves, LANES), f32),
            pltpu.VMEM((depth, LANES), f32),
            pltpu.VMEM((n_ja, gram_rows, LANES), f32),
            pltpu.VMEM((n_ka, gram_rows, LANES), f32),
            pltpu.VMEM((n_ia, gram_rows, LANES), f32),
            pltpu.VMEM((n_ka, one_rows, LANES), f32),
            pltpu.VMEM((n_ja, one_rows, LANES), f32),
            pltpu.VMEM((n_mix, two_rows, LANES), f32),
            dma((chunks * halves,)),
            dma((3,)),
            *pair(n_ja), *pair(n_ka), *pair(n_ia), *pair(n_ka), *pair(n_ja), *pair(n_mix),
        ],
        compiler_params=pltpu.CompilerParams(collective_id=0, has_side_effects=True),
        name="als_sweep",
    )(
        tensor.reshape(rows_first * depth, rows_third), factor_two.T, factor_three.T, factor_four
    )
    def hand_on(one_ref, two_ref, one_out, two_out):
        one_out[...] = one_ref[...]
        two_out[...] = two_ref[...]

    one_t, two_t = pl.pallas_call(
        hand_on,
        out_shape=(
            jax.ShapeDtypeStruct((rank, rows_first), f32),
            jax.ShapeDtypeStruct((rank, rows_second), f32),
        ),
        in_specs=[pl.BlockSpec(memory_space=pltpu.VMEM)] * 2,
        out_specs=(pl.BlockSpec(memory_space=pltpu.VMEM),) * 2,
        compiler_params=pltpu.CompilerParams(vmem_limit_bytes=2 * 1024 * 1024),
        name="hand_on",
    )(one_t, two_t)
    return one_t.T, two_t.T


def solution(mesh):
    return jax.shard_map(
        functools.partial(per_device, mesh.shape["ia"], mesh.shape["ja"], mesh.shape["ka"]),
        mesh=mesh,
        in_specs=(P("ia", "ja", None, "ka"), P("ja", None), P("ka", None), P()),
        out_specs=(P("ia", None), P("ja", None)),
        check_vma=False,
    )
```
